32 devices in a mesh: groups: 2 (over x), seq: 4 (over y, core), head: 4 (over z).
Axes of the slice: x: 2, y: 2, z: 4, core: 2. Of those that a mesh axis runs over, the one named last changes fastest.
Arguments:
- query: bfloat16 [32, 16, 1024], P('groups', None, 'head'), parts along dimension 0, may hold values from -6 to 6, as said below
- new_key: bfloat16 [32, 16, 1024], P('groups', None, 'head'), parts along dimension 0, may hold values from -6 to 6
- new_value: bfloat16 [32, 16, 1024], P('groups', None, 'head'), parts along dimension 0, may hold values from -6 to 6
- keys: bfloat16 [32, 4096, 1024], P('groups', 'seq', 'head'), parts along dimension 0, may hold values from -6 to 6, as said below
- values: bfloat16 [32, 4096, 1024], P('groups', 'seq', 'head'), parts along dimension 0, may hold values from -6 to 6
- lengths: int32 [32], P('groups'), parts along dimension 0, may hold values from 2 to 4096
- time_bucket: int32 [32, 4096], P('groups', 'seq'), parts along dimension 0, may hold values from 0 to 63
- action: int32 [32, 4096], P('groups', 'seq'), parts along dimension 0, may hold values from 0 to 15
- time_bias: float32 [64, 8], P(None, 'head'), may hold values from -0.25 to 0.25
- action_bias: float32 [16, 8], P(None, 'head'), may hold values from -0.25 to 0.25
- gate: bfloat16 [32, 16, 1024], P('groups', None, 'head'), parts along dimension 0, may hold values from -6 to 6
- norm_gain: float32 [1024], P('head'), may hold values from 0.1 to 1.9
- w_out: bfloat16 [1024, 1024], P('head'), may hold values from -0.1875 to 0.1875
Outputs:
- output: bfloat16 [32, 16, 1024], P(('groups', 'seq'), None, 'head'), parts along dimension 0
The draws below stay inside these ranges and needn't reach their ends.
There are 2 independent parts, one for each index of `groups`. The reference program is written for one: setup_inputs(seed, part) draws one part's arguments, and reference() takes and returns one part's arrays. A program takes and returns all parts, laid end to end along the dimension named above; an argument that names none is the same for every part. Nothing has to cross between parts.
Inputs may be any that keep to these rules, and one draw needn't show every extreme that they name: `query`: queries of order one; some users' queries may be large and equal to some of their keys. `keys`: keys of order one.
All inputs are finite; a program needn't handle non-finite values.
Results may differ from the reference program's by a relative error of at most 0.0056.
Values sent between devices are 32-bit elements; how exact they have to be, the bound alone decides.
No kernel may reach another device: no remote copies, remote signals or barrier semaphores. Data moves between devices by JAX's collectives and lax.ppermute only.
A program may use at most 64 MiB of HBM per device.

```python
import math
import jax
import jax.numpy as jnp
from jax import lax

USERS = 16
CANDS = 16
S_DEV = 1024
HEADS = 8
DH = 128
D_MODEL = 1024
BUCKETS = 64
ACTIONS = 16
HISTORY = 4096
N_SEQ = 4


def draw_query(key, part):
    result = jax.random.truncated_normal(jax.random.fold_in(key, 1), -6.0, 6.0, (USERS, CANDS, HEADS * DH), jnp.float32)
    return result.astype(jnp.bfloat16)


def draw_keys(key, part):
    result = jax.random.truncated_normal(jax.random.fold_in(key, 2), -6.0, 6.0, (USERS, HISTORY, HEADS * DH), jnp.float32)
    return result.astype(jnp.bfloat16)


def plant(values, key, smallest, top_value):
    place = [jax.random.randint(jax.random.fold_in(key, axis), (), 0, length) for axis, length in enumerate(values.shape)]
    widest = values.shape.index(max(values.shape))
    beside = place[:widest] + [(place[widest] + 1) % values.shape[widest]] + place[widest + 1:]
    return values.at[tuple(place)].set(smallest).at[tuple(beside)].set(top_value)


def block_levels(key, dims, split, least, largest):
    def one(dim, blocks):
        steps = jax.random.uniform(jax.random.fold_in(jax.random.fold_in(key, 6), dim), (blocks,), jnp.float32, least / len(split), largest / len(split))
        return jnp.repeat(jnp.exp(steps), dims[dim] // blocks).reshape((-1,) + (1,) * (len(dims) - dim - 1))

    gain = one(*split[0])
    for cut in split[1:]:
        gain = gain * one(*cut)
    return gain


def noise(stream_key, extent, scale, bound, split=(), held_as=jnp.bfloat16):
    values = scale * jax.random.normal(stream_key, extent, jnp.float32)
    if split:
        values = values * block_levels(stream_key, extent, split, -0.22, 0.18)
    return jnp.clip(values, -bound, bound).astype(held_as)


def setup_inputs(seed: int = 0, part: int = 0) -> dict:
    splits = jax.random.split(jax.random.key(seed), 14)
    own_keys = jax.random.split(jax.random.fold_in(splits[13], part), 14)
    return {
        "query": draw_query(jax.random.fold_in(jax.random.fold_in(splits[13], part), 71), part),
        "new_key": noise(own_keys[1], (USERS, CANDS, HEADS * DH), 1.0, 6.0, ((2, 4),)),
        "new_value": noise(own_keys[2], (USERS, CANDS, HEADS * DH), 1.0, 6.0, ((2, 4),)),
        "keys": draw_keys(jax.random.fold_in(jax.random.fold_in(splits[13], part), 71), part),
        "values": noise(own_keys[4], (USERS, HISTORY, HEADS * DH), 1.0, 6.0, ((1, 4), (2, 4))),
        "lengths": plant(jax.random.randint(own_keys[5], (USERS,), 2, HISTORY + 1), jax.random.fold_in(own_keys[5], 1), 2, HISTORY).astype(jnp.int32),
        "time_bucket": plant(jax.random.randint(own_keys[6], (USERS, HISTORY), 0, BUCKETS), jax.random.fold_in(own_keys[6], 1), 0, BUCKETS - 1).astype(jnp.int32),
        "action": plant(jax.random.randint(own_keys[7], (USERS, HISTORY), 0, ACTIONS), jax.random.fold_in(own_keys[7], 1), 0, ACTIONS - 1).astype(jnp.int32),
        "time_bias": jnp.clip(jax.random.uniform(splits[8], (BUCKETS, HEADS), jnp.float32, -0.25, 0.25) * block_levels(splits[8], (BUCKETS, HEADS), ((1, 4),), -0.4, 0.0), -0.25, 0.25),
        "action_bias": jnp.clip(jax.random.uniform(splits[9], (ACTIONS, HEADS), jnp.float32, -0.25, 0.25) * block_levels(splits[9], (ACTIONS, HEADS), ((1, 4),), -0.4, 0.0), -0.25, 0.25),
        "gate": noise(own_keys[10], (USERS, CANDS, HEADS * DH), 1.0, 6.0, ((2, 4),)),
        "norm_gain": jnp.clip(1.0 + 0.18 * jax.random.normal(splits[11], (HEADS * DH,), jnp.float32), 0.1, 1.9),
        "w_out": noise(splits[12], (HEADS * DH, D_MODEL), (HEADS * DH) ** -0.5, 0.1875, ((0, 4),)),
    }


def reference(query, new_key, new_value, keys, values, lengths, time_bucket, action, time_bias, action_bias, gate, norm_gain, w_out):
    user_count = keys.shape[0]
    cand_count = query.shape[1]
    head_count = HEADS
    head_size = DH
    score_scale = 1.0 / math.sqrt(head_size)
    query_heads = query.astype(jnp.float32).reshape(user_count, cand_count, head_count, head_size)

    def one_block(block_index):
        first = (block_index * S_DEV).astype(jnp.int32)
        key_block = lax.dynamic_slice_in_dim(keys, first, S_DEV, 1).astype(jnp.float32).reshape(user_count, S_DEV, head_count, head_size)
        value_block = lax.dynamic_slice_in_dim(values, first, S_DEV, 1).astype(jnp.float32).reshape(user_count, S_DEV, head_count, head_size)
        bucket_block = lax.dynamic_slice_in_dim(time_bucket, first, S_DEV, 1)
        action_block = lax.dynamic_slice_in_dim(action, first, S_DEV, 1)
        scores = jnp.einsum('uchd,ushd->uchs', query_heads, key_block) * score_scale
        biases = jnp.transpose(time_bias[bucket_block], (0, 2, 1)) + jnp.transpose(action_bias[action_block], (0, 2, 1))
        scores = scores + biases[:, None]
        position = first + jnp.arange(S_DEV, dtype=jnp.int32)
        valid = position[None, None, None, :] < lengths[:, None, None, None]
        block_max = lax.optimization_barrier(jnp.max(jnp.where(valid, scores, -1e+30), axis=-1))
        weights = jnp.where(valid, jnp.exp(scores - block_max[..., None]), 0.0)
        block_sum = lax.optimization_barrier(jnp.sum(weights, axis=-1))
        rounded = weights.astype(jnp.bfloat16).astype(jnp.float32)
        block_acc = jnp.einsum('uchs,ushd->uchd', rounded, value_block)
        return (block_max, block_sum, block_acc)
    maxima, sums, accs = lax.map(one_block, jnp.arange(N_SEQ, dtype=jnp.int32))
    own = lax.optimization_barrier(jnp.sum(query_heads * new_key.astype(jnp.float32).reshape(user_count, cand_count, head_count, head_size), axis=-1)) * score_scale
    overall = jnp.maximum(lax.optimization_barrier(jnp.max(maxima, axis=0)), own)
    factors = jnp.exp(maxima - overall[None])
    own_factor = jnp.exp(own - overall)
    numer = lax.optimization_barrier(jnp.sum(factors[..., None] * accs, axis=0)) + own_factor[..., None] * new_value.astype(jnp.float32).reshape(user_count, cand_count, head_count, head_size)
    denom = lax.optimization_barrier(jnp.sum(factors * sums, axis=0)) + own_factor
    attended = numer / denom[..., None]
    square_sum = lax.optimization_barrier(jnp.sum(jnp.square(attended), axis=(2, 3)))
    gate_heads = gate.astype(jnp.float32).reshape(user_count, cand_count, head_count, head_size)
    hidden = (attended * norm_gain.reshape(head_count, head_size) * jax.nn.silu(gate_heads)).astype(jnp.bfloat16)
    hidden = hidden.reshape(user_count * cand_count, head_count * head_size)
    projected = jnp.dot(hidden, w_out, preferred_element_type=jnp.float32).reshape(user_count, cand_count, -1)
    factor = 1.0 / jnp.sqrt(square_sum / (head_count * head_size) + 1e-06)
    return (projected * factor[:, :, None]).astype(jnp.bfloat16)
```

```python
import functools
import math

import jax
import jax.numpy as jnp
from jax import lax
from jax.experimental import pallas as pl
from jax.experimental.pallas import tpu as pltpu
from jax.sharding import PartitionSpec as P

LANES = 128
SUBLANES = 8
MASKED = -1e30
HALF = LANES // 2


def column_to_row(column, first_lane):
    rows = column.shape[0]
    row_id = lax.broadcasted_iota(jnp.int32, (rows, LANES), 0)
    lane_id = lax.broadcasted_iota(jnp.int32, (rows, LANES), 1)
    return jnp.sum(
        jnp.where(lane_id == row_id + first_lane, column, 0.0), axis=0, keepdims=True
    )


def attend_kernel(
    query_hbm,
    new_key_hbm,
    new_value_hbm,
    keys_hbm,
    values_hbm,
    lengths_hbm,
    time_bucket_hbm,
    action_hbm,
    time_bias_hbm,
    action_bias_hbm,
    gate_hbm,
    gain_hbm,
    packed_ref,
    self_ref,
    gated_ref,
    key_buf,
    value_buf,
    query_buf,
    new_key_buf,
    new_value_buf,
    gate_buf,
    gain_buf,
    bucket_buf,
    action_buf,
    time_table,
    action_table,
    bias_buf,
    lengths_smem,
    block_sems,
    small_sems,
    *,
    unroll,
):
    users, block_len, width = key_buf.shape
    cands = query_buf.shape[1]
    head_count = time_table.shape[0]
    head_size = width // head_count
    group_rows = head_count * cands
    seq_count = packed_ref.shape[0]
    local_users = users // seq_count
    stat_row = local_users * group_rows
    scale = 1.0 / math.sqrt(head_size)
    rank = lax.axis_index("seq")
    first_user = rank * local_users

    small = [
        pltpu.make_async_copy(source, target, small_sems.at[number])
        for number, (source, target) in enumerate(
            [
                (lengths_hbm, lengths_smem),
                (time_bias_hbm, time_table),
                (action_bias_hbm, action_table),
                (time_bucket_hbm, bucket_buf),
                (action_hbm, action_buf),
                (query_hbm, query_buf),
                (new_key_hbm.at[pl.ds(first_user, local_users)], new_key_buf),
                (new_value_hbm.at[pl.ds(first_user, local_users)], new_value_buf),
                (gate_hbm.at[pl.ds(first_user, local_users)], gate_buf),
                (gain_hbm, gain_buf),
            ]
        )
    ]

    def key_copy(user):
        return pltpu.make_async_copy(keys_hbm.at[user], key_buf.at[user], block_sems.at[0, user])

    def value_copy(user):
        return pltpu.make_async_copy(
            values_hbm.at[user], value_buf.at[user], block_sems.at[1, user]
        )

    for copy in small[:6]:
        copy.start()
    for user in range(users):
        key_copy(user).start()
        value_copy(user).start()
    for copy in small[6:]:
        copy.start()
    for copy in small[:6]:
        copy.wait()

    lane_id = lax.broadcasted_iota(jnp.int32, (SUBLANES, LANES), 1)
    sub_id = lax.broadcasted_iota(jnp.int32, (SUBLANES, LANES), 0)

    def padded_table(ref, head):
        row = ref[head : head + 1, :]
        missing = LANES - row.shape[1]
        row = jnp.concatenate([row, jnp.zeros((1, missing), row.dtype)], axis=1)
        return jnp.broadcast_to(row, (SUBLANES, LANES))

    time_rows = [padded_table(time_table, head) for head in range(head_count)]
    action_rows = [padded_table(action_table, head) for head in range(head_count)]
    for group in range(users // SUBLANES):
        limit = jnp.zeros((SUBLANES, LANES), jnp.int32)
        for member in range(SUBLANES):
            left = lengths_smem[group * SUBLANES + member] - rank * block_len
            limit = jnp.where(sub_id == member, left, limit)
        rows = slice(group * SUBLANES, (group + 1) * SUBLANES)
        for piece in range(block_len // LANES):
            cols = slice(piece * LANES, (piece + 1) * LANES)
            bucket = bucket_buf[rows, cols]
            kind = action_buf[rows, cols]
            valid = lane_id + piece * LANES < limit
            for head in range(head_count):
                bias = jnp.take_along_axis(
                    time_rows[head], bucket, axis=1, mode="promise_in_bounds"
                ) + jnp.take_along_axis(
                    action_rows[head], kind, axis=1, mode="promise_in_bounds"
                )
                bias_buf[head, rows, cols] = jnp.where(valid, bias, MASKED)

    col_head = lax.broadcasted_iota(jnp.int32, (cands, width), 1) // head_size

    def one_user(user):
        key_copy(user).wait()
        query = query_buf[user]
        stacked = jnp.concatenate(
            [
                jnp.where(col_head == head, query, jnp.zeros_like(query))
                for head in range(head_count)
            ],
            axis=0,
        )
        scores = lax.dot_general(
            stacked,
            key_buf[user],
            (((1,), (1,)), ((), ())),
            preferred_element_type=jnp.float32,
        )
        biases = jnp.concatenate(
            [
                jnp.broadcast_to(bias_buf[head, pl.ds(user, 1), :], (cands, block_len))
                for head in range(head_count)
            ],
            axis=0,
        )
        scores = scores * scale + biases
        block_max = jnp.max(scores, axis=1, keepdims=True)
        weights = jnp.exp(scores - block_max)
        block_sum = jnp.sum(weights, axis=1, keepdims=True)
        value_copy(user).wait()
        block_acc = jnp.dot(
            weights.astype(jnp.bfloat16), value_buf[user], preferred_element_type=jnp.float32
        )
        target = user // local_users
        place = user % local_users
        for head in range(head_count):
            packed_ref[
                target, pl.ds(pl.multiple_of(place * group_rows + head * cands, SUBLANES), cands), :
            ] = block_acc[
                head * cands : (head + 1) * cands, head * head_size : (head + 1) * head_size
            ]
        packed_ref[target, pl.ds(stat_row + place, 1), :] = column_to_row(
            block_max, 0
        ) + column_to_row(block_sum, HALF)

    def several(step, carry):
        for member in range(unroll):
            one_user(step * unroll + member)
        return carry

    lax.fori_loop(0, users // unroll, several, 0)

    for copy in small[6:]:
        copy.wait()
    gain = gain_buf[...].reshape(1, width)
    for place in range(local_users):
        own_query = query_buf[first_user + place].astype(jnp.float32)
        own_key = new_key_buf[place].astype(jnp.float32)
        own_value = new_value_buf[place].astype(jnp.float32)
        gate = gate_buf[place].astype(jnp.float32)
        product = own_query * own_key
        row = jnp.zeros((1, LANES), jnp.float32)
        for head in range(head_count):
            cols = slice(head * head_size, (head + 1) * head_size)
            own = jnp.sum(product[:, cols], axis=1, keepdims=True) * scale
            row = row + column_to_row(own, head * cands)
            row = row + column_to_row(jnp.ones_like(own), HALF + head * cands)
            first = place * group_rows + head * cands
            self_ref[first : first + cands, :] = own_value[:, cols]
        self_ref[stat_row + place : stat_row + place + 1, :] = row
        gated_ref[place * cands : (place + 1) * cands, :] = gain * (gate / (1.0 + jnp.exp(-gate)))


def project_kernel(packed_ref, self_ref, gated_ref, w_ref, send_ref, *, cands):
    seq_count, _, head_size = packed_ref.shape
    row_count, width = gated_ref.shape
    head_count = width // head_size
    local_users = row_count // cands
    group_rows = head_count * cands
    stat_row = local_users * group_rows
    dest_count, _, out_cols = send_ref.shape
    sources = seq_count + 1

    stats = []
    for place in range(local_users):
        for source in range(seq_count):
            stats.append(packed_ref[source, stat_row + place : stat_row + place + 1, :])
        stats.append(self_ref[stat_row + place : stat_row + place + 1, :])
    missing = LANES - len(stats)
    stats.append(jnp.zeros((missing, LANES), jnp.float32))
    columns = jnp.concatenate(stats, axis=0).T

    hidden = []
    square_row = jnp.zeros((1, LANES), jnp.float32)
    for place in range(local_users):
        span = slice(place * sources, (place + 1) * sources)
        maxima = columns[0:group_rows, span]
        sums = columns[HALF : HALF + group_rows, span]
        top = jnp.max(maxima, axis=1, keepdims=True)
        factors = jnp.exp(maxima - top)
        factors = factors / jnp.sum(factors * sums, axis=1, keepdims=True)
        rows = slice(place * group_rows, (place + 1) * group_rows)
        attended = factors[:, seq_count:] * self_ref[rows, :]
        for source in range(seq_count):
            attended = attended + factors[:, source : source + 1] * packed_ref[source, rows, :]
        wide = jnp.concatenate(
            [attended[head * cands : (head + 1) * cands, :] for head in range(head_count)], axis=1
        )
        square = jnp.sum(wide * wide, axis=1, keepdims=True)
        square_row = square_row + column_to_row(square, place * cands)
        gated = gated_ref[place * cands : (place + 1) * cands, :]
        hidden.append((wide * gated).astype(jnp.bfloat16))
    projected = jnp.dot(
        jnp.concatenate(hidden, axis=0), w_ref[...], preferred_element_type=jnp.float32
    )
    for dest in range(dest_count):
        send_ref[dest, 0:row_count, :] = projected[:, dest * out_cols : (dest + 1) * out_cols]
        send_ref[dest, row_count : row_count + 1, 0:LANES] = square_row


def finish_kernel(parts_ref, out_ref, *, full_width):
    head_axis, _, out_cols = parts_ref.shape
    local_users, cands, _ = out_ref.shape
    row_count = local_users * cands
    total = parts_ref[0, 0:row_count, :]
    square_row = parts_ref[0, row_count : row_count + 1, 0:LANES]
    for source in range(1, head_axis):
        total = total + parts_ref[source, 0:row_count, :]
        square_row = square_row + parts_ref[source, row_count : row_count + 1, 0:LANES]
    row_id = lax.broadcasted_iota(jnp.int32, (row_count, LANES), 0)
    lane_id = lax.broadcasted_iota(jnp.int32, (row_count, LANES), 1)
    squares = jnp.sum(jnp.where(lane_id == row_id, square_row, 0.0), axis=1, keepdims=True)
    factor = 1.0 / jnp.sqrt(squares / full_width + 1e-06)
    result = (total * factor).astype(out_ref.dtype)
    for place in range(local_users):
        out_ref[place] = result[place * cands : (place + 1) * cands, :]


def body(
    query,
    new_key,
    new_value,
    keys,
    values,
    lengths,
    time_bucket,
    action,
    time_bias,
    action_bias,
    gate,
    norm_gain,
    w_out,
):
    users, block_len, width = keys.shape
    cands = query.shape[1]
    head_count = time_bias.shape[1]
    head_size = width // head_count
    seq_count = lax.axis_size("seq")
    head_axis = lax.axis_size("head")
    local_users = users // seq_count
    row_count = local_users * cands
    group_rows = head_count * cands
    packet_rows = local_users * group_rows + SUBLANES
    out_cols = w_out.shape[1] // head_axis
    f32 = jnp.float32
    any_spec = pl.BlockSpec(memory_space=pl.ANY)
    vmem_spec = pl.BlockSpec(memory_space=pltpu.VMEM)

    packed, own, gated = pl.pallas_call(
        functools.partial(attend_kernel, unroll=4),
        out_shape=(
            jax.ShapeDtypeStruct((seq_count, packet_rows, head_size), f32),
            jax.ShapeDtypeStruct((packet_rows, head_size), f32),
            jax.ShapeDtypeStruct((row_count, width), f32),
        ),
        in_specs=[any_spec] * 12,
        out_specs=(vmem_spec, vmem_spec, vmem_spec),
        scratch_shapes=[
            pltpu.VMEM(keys.shape, keys.dtype),
            pltpu.VMEM(values.shape, values.dtype),
            pltpu.VMEM(query.shape, query.dtype),
            pltpu.VMEM((local_users, cands, width), new_key.dtype),
            pltpu.VMEM((local_users, cands, width), new_value.dtype),
            pltpu.VMEM((local_users, cands, width), gate.dtype),
            pltpu.VMEM(norm_gain.shape, f32),
            pltpu.VMEM(time_bucket.shape, jnp.int32),
            pltpu.VMEM(action.shape, jnp.int32),
            pltpu.VMEM(time_bias.shape[::-1], f32),
            pltpu.VMEM(action_bias.shape[::-1], f32),
            pltpu.VMEM((head_count, users, block_len), f32),
            pltpu.SMEM(lengths.shape, jnp.int32),
            pltpu.SemaphoreType.DMA((2, users)),
            pltpu.SemaphoreType.DMA((10,)),
        ],
        name="attend",
    )(
        query,
        new_key,
        new_value,
        keys,
        values,
        lengths,
        time_bucket,
        action,
        time_bias.T,
        action_bias.T,
        gate,
        norm_gain,
    )
    received = lax.all_to_all(packed, "seq", split_axis=0, concat_axis=0, tiled=True)
    sent = pl.pallas_call(
        functools.partial(project_kernel, cands=cands),
        out_shape=jax.ShapeDtypeStruct((head_axis, row_count + SUBLANES, out_cols), f32),
        in_specs=[vmem_spec] * 4,
        out_specs=vmem_spec,
        name="project",
    )(received, own, gated, w_out)
    parts = lax.all_to_all(sent, "head", split_axis=0, concat_axis=0, tiled=True)
    return pl.pallas_call(
        functools.partial(finish_kernel, full_width=width * head_axis),
        out_shape=jax.ShapeDtypeStruct((local_users, cands, out_cols), jnp.bfloat16),
        in_specs=[vmem_spec],
        out_specs=vmem_spec,
        name="finish",
    )(parts)


def solution(mesh):
    placed = (
        P("groups", None, "head"),
        P("groups", None, "head"),
        P("groups", None, "head"),
        P("groups", "seq", "head"),
        P("groups", "seq", "head"),
        P("groups"),
        P("groups", "seq"),
        P("groups", "seq"),
        P(None, "head"),
        P(None, "head"),
        P("groups", None, "head"),
        P("head"),
        P("head", None),
    )
    return jax.shard_map(
        body,
        mesh=mesh,
        in_specs=placed,
        out_specs=P(("groups", "seq"), None, "head"),
        check_vma=False,
    )
```

```python
import functools
import math

import jax
import jax.numpy as jnp
from jax import lax
from jax.experimental import pallas as pl
from jax.experimental.pallas import tpu as pltpu
from jax.sharding import PartitionSpec as P

LANES = 128
SUBLANES = 8
MASKED = -1e30
HALF = LANES // 2
STEP_USERS = 4
AHEAD = 2
SPLIT = False


def partner_of(rank, offset, size):
    if size & (size - 1) == 0:
        return rank ^ offset
    return (rank + offset) % size


def exchange(packet, axis, offset):
    size = lax.axis_size(axis)
    pairs = [(rank, partner_of(rank, offset, size)) for rank in range(size)]
    return lax.ppermute(packet, axis, pairs)


def column_to_row(column, first_lane):
    rows = column.shape[0]
    row_id = lax.broadcasted_iota(jnp.int32, (rows, LANES), 0)
    lane_id = lax.broadcasted_iota(jnp.int32, (rows, LANES), 1)
    return jnp.sum(
        jnp.where(lane_id == row_id + first_lane, column, 0.0), axis=0, keepdims=True
    )


def attend_kernel(*refs, offsets, seq_count, with_own, step_users, ahead):
    refs = list(refs)
    take = lambda count: [refs.pop(0) for _ in range(count)]
    (
        query_hbm,
        keys_hbm,
        values_hbm,
        lengths_hbm,
        time_bucket_hbm,
        action_hbm,
        time_bias_hbm,
        action_bias_hbm,
    ) = take(8)
    if with_own:
        new_key_hbm, new_value_hbm, gate_hbm, gain_hbm = take(4)
    packets = take(len(offsets))
    if with_own:
        self_ref, gated_ref = take(2)
    (
        key_buf,
        value_buf,
        query_buf,
        bucket_buf,
        action_buf,
        time_table,
        action_table,
        bias_buf,
        lengths_smem,
        block_sems,
        small_sems,
    ) = take(11)
    if with_own:
        new_key_buf, new_value_buf, gate_buf, gain_buf, own_sems = take(5)
    _, block_len, width = key_buf.shape
    users, cands, _ = query_buf.shape
    head_count = time_table.shape[0]
    head_size = width // head_count
    group_rows = head_count * cands
    local_users = users // seq_count
    stat_row = local_users * group_rows
    scale = 1.0 / math.sqrt(head_size)
    rank = lax.axis_index("seq")
    first_user = rank * local_users

    small = [
        pltpu.make_async_copy(source, target, small_sems.at[number])
        for number, (source, target) in enumerate(
            [
                (lengths_hbm, lengths_smem),
                (time_bias_hbm, time_table),
                (action_bias_hbm, action_table),
                (time_bucket_hbm, bucket_buf),
                (action_hbm, action_buf),
                (query_hbm, query_buf),
            ]
        )
    ]
    late = []
    if with_own:
        own_rows = pl.ds(first_user, local_users)
        late = [
            pltpu.make_async_copy(source, target, own_sems.at[number])
            for number, (source, target) in enumerate(
                [
                    (new_key_hbm.at[own_rows], new_key_buf),
                    (new_value_hbm.at[own_rows], new_value_buf),
                    (gate_hbm.at[own_rows], gate_buf),
                    (gain_hbm, gain_buf),
                ]
            )
        ]

    steps = [
        (slot, place)
        for slot in range(len(offsets))
        for place in range(0, local_users, step_users)
    ]

    def copies(number):
        slot, place = steps[number]
        source = pl.ds(
            partner_of(rank, offsets[slot], seq_count) * local_users + place, step_users
        )
        target = pl.ds(number * step_users, step_users)
        return (
            pltpu.make_async_copy(
                keys_hbm.at[source], key_buf.at[target], block_sems.at[0, number]
            ),
            pltpu.make_async_copy(
                values_hbm.at[source], value_buf.at[target], block_sems.at[1, number]
            ),
        )

    for copy in small:
        copy.start()
    for number in range(min(ahead, len(steps))):
        for copy in copies(number):
            copy.start()
    for copy in late:
        copy.start()
    for copy in small:
        copy.wait()

    lane_id = lax.broadcasted_iota(jnp.int32, (SUBLANES, LANES), 1)
    sub_id = lax.broadcasted_iota(jnp.int32, (SUBLANES, LANES), 0)

    def padded_table(ref, head):
        row = ref[head : head + 1, :]
        missing = LANES - row.shape[1]
        row = jnp.concatenate([row, jnp.zeros((1, missing), row.dtype)], axis=1)
        return jnp.broadcast_to(row, (SUBLANES, LANES))

    time_rows = [padded_table(time_table, head) for head in range(head_count)]
    action_rows = [padded_table(action_table, head) for head in range(head_count)]
    for group in range(users // SUBLANES):
        limit = jnp.zeros((SUBLANES, LANES), jnp.int32)
        for member in range(SUBLANES):
            left = lengths_smem[group * SUBLANES + member] - rank * block_len
            limit = jnp.where(sub_id == member, left, limit)
        rows = slice(group * SUBLANES, (group + 1) * SUBLANES)
        for piece in range(block_len // LANES):
            cols = slice(piece * LANES, (piece + 1) * LANES)
            bucket = bucket_buf[rows, cols]
            kind = action_buf[rows, cols]
            valid = lane_id + piece * LANES < limit
            for head in range(head_count):
                bias = jnp.take_along_axis(
                    time_rows[head], bucket, axis=1, mode="promise_in_bounds"
                ) + jnp.take_along_axis(
                    action_rows[head], kind, axis=1, mode="promise_in_bounds"
                )
                bias_buf[head, rows, cols] = jnp.where(valid, bias, MASKED)

    col_head = lax.broadcasted_iota(jnp.int32, (cands, width), 1) // head_size

    def one_user(slot, place, held):
        user = partner_of(rank, offsets[slot], seq_count) * local_users + place
        query = query_buf[user]
        stacked = jnp.concatenate(
            [
                jnp.where(col_head == head, query, jnp.zeros_like(query))
                for head in range(head_count)
            ],
            axis=0,
        )
        scores = lax.dot_general(
            stacked,
            key_buf[held],
            (((1,), (1,)), ((), ())),
            preferred_element_type=jnp.float32,
        )
        biases = jnp.concatenate(
            [
                jnp.broadcast_to(bias_buf[head, pl.ds(user, 1), :], (cands, block_len))
                for head in range(head_count)
            ],
            axis=0,
        )
        scores = scores * scale + biases
        block_max = jnp.max(scores, axis=1, keepdims=True)
        weights = jnp.exp(scores - block_max)
        block_sum = jnp.sum(weights, axis=1, keepdims=True)
        block_acc = jnp.dot(
            weights.astype(jnp.bfloat16), value_buf[held], preferred_element_type=jnp.float32
        )
        packet = packets[slot]
        for head in range(head_count):
            first = place * group_rows + head * cands
            packet[first : first + cands, :] = block_acc[
                head * cands : (head + 1) * cands, head * head_size : (head + 1) * head_size
            ]
        packet[stat_row + place : stat_row + place + 1, :] = column_to_row(
            block_max, 0
        ) + column_to_row(block_sum, HALF)

    for number, (slot, place) in enumerate(steps):
        for copy in copies(number):
            copy.wait()
        if number + ahead < len(steps):
            for copy in copies(number + ahead):
                copy.start()
        for member in range(step_users):
            one_user(slot, place + member, number * step_users + member)

    if not with_own:
        return
    for copy in late:
        copy.wait()
    gain = gain_buf[...].reshape(1, width)
    for place in range(local_users):
        own_query = query_buf[first_user + place].astype(jnp.float32)
        own_key = new_key_buf[place].astype(jnp.float32)
        own_value = new_value_buf[place].astype(jnp.float32)
        gate = gate_buf[place].astype(jnp.float32)
        product = own_query * own_key
        row = jnp.zeros((1, LANES), jnp.float32)
        for head in range(head_count):
            cols = slice(head * head_size, (head + 1) * head_size)
            own = jnp.sum(product[:, cols], axis=1, keepdims=True) * scale
            row = row + column_to_row(own, head * cands)
            row = row + column_to_row(jnp.ones_like(own), HALF + head * cands)
            first = place * group_rows + head * cands
            self_ref[first : first + cands, :] = own_value[:, cols]
        self_ref[stat_row + place : stat_row + place + 1, :] = row
        gated_ref[place * cands : (place + 1) * cands, :] = gain * (gate / (1.0 + jnp.exp(-gate)))


def project_kernel(*refs, cands, source_count, head_axis):
    packets = refs[:source_count]
    gated_ref, w_ref = refs[source_count : source_count + 2]
    sends = refs[source_count + 2 :]
    head_size = packets[0].shape[1]
    row_count, width = gated_ref.shape
    head_count = width // head_size
    local_users = row_count // cands
    group_rows = head_count * cands
    stat_row = local_users * group_rows
    out_cols = w_ref.shape[1] // head_axis
    rank = lax.axis_index("head")

    stats = [
        packet[stat_row + place : stat_row + place + 1, :]
        for place in range(local_users)
        for packet in packets
    ]
    stats.append(jnp.zeros((LANES - len(stats), LANES), jnp.float32))
    columns = jnp.concatenate(stats, axis=0).T

    hidden = []
    square_row = jnp.zeros((1, LANES), jnp.float32)
    for place in range(local_users):
        span = slice(place * source_count, (place + 1) * source_count)
        maxima = columns[0:group_rows, span]
        sums = columns[HALF : HALF + group_rows, span]
        top = jnp.max(maxima, axis=1, keepdims=True)
        factors = jnp.exp(maxima - top)
        factors = factors / jnp.sum(factors * sums, axis=1, keepdims=True)
        rows = slice(place * group_rows, (place + 1) * group_rows)
        attended = factors[:, 0:1] * packets[0][rows, :]
        for source in range(1, source_count):
            attended = attended + factors[:, source : source + 1] * packets[source][rows, :]
        wide = jnp.concatenate(
            [attended[head * cands : (head + 1) * cands, :] for head in range(head_count)], axis=1
        )
        square = jnp.sum(wide * wide, axis=1, keepdims=True)
        square_row = square_row + column_to_row(square, place * cands)
        gated = gated_ref[place * cands : (place + 1) * cands, :]
        hidden.append((wide * gated).astype(jnp.bfloat16))
    hidden = jnp.concatenate(hidden, axis=0)
    for offset in reversed(range(head_axis)):
        first = pl.multiple_of(partner_of(rank, offset, head_axis) * out_cols, LANES)
        sends[offset][0:row_count, :] = jnp.dot(
            hidden, w_ref[:, pl.ds(first, out_cols)], preferred_element_type=jnp.float32
        )
        sends[offset][row_count : row_count + 1, 0:LANES] = square_row


def finish_kernel(*refs, full_width):
    parts, out_ref = refs[:-1], refs[-1]
    local_users, cands, _ = out_ref.shape
    row_count = local_users * cands
    total = parts[0][0:row_count, :]
    square_row = parts[0][row_count : row_count + 1, 0:LANES]
    for part in parts[1:]:
        total = total + part[0:row_count, :]
        square_row = square_row + part[row_count : row_count + 1, 0:LANES]
    row_id = lax.broadcasted_iota(jnp.int32, (row_count, LANES), 0)
    lane_id = lax.broadcasted_iota(jnp.int32, (row_count, LANES), 1)
    squares = jnp.sum(jnp.where(lane_id == row_id, square_row, 0.0), axis=1, keepdims=True)
    factor = 1.0 / jnp.sqrt(squares / full_width + 1e-06)
    result = (total * factor).astype(out_ref.dtype)
    for place in range(local_users):
        out_ref[place] = result[place * cands : (place + 1) * cands, :]


def body(
    query,
    new_key,
    new_value,
    keys,
    values,
    lengths,
    time_bucket,
    action,
    time_bias,
    action_bias,
    gate,
    norm_gain,
    w_out,
):
    users, block_len, width = keys.shape
    cands = query.shape[1]
    head_count = time_bias.shape[1]
    head_size = width // head_count
    seq_count = lax.axis_size("seq")
    head_axis = lax.axis_size("head")
    local_users = users // seq_count
    row_count = local_users * cands
    packet_rows = local_users * head_count * cands + SUBLANES
    out_cols = w_out.shape[1] // head_axis
    f32 = jnp.float32
    hbm_spec = pl.BlockSpec(memory_space=pltpu.HBM)
    vmem_spec = pl.BlockSpec(memory_space=pltpu.VMEM)
    packet_shape = jax.ShapeDtypeStruct((packet_rows, head_size), f32)
    step_users = math.gcd(local_users, STEP_USERS)

    def attend(offsets, with_own):
        held = len(offsets) * local_users
        steps = held // step_users
        held_bytes = 2 * held * block_len * width * keys.dtype.itemsize
        operands = [
            query, keys, values, lengths, time_bucket, action, time_bias.T, action_bias.T
        ]
        outputs = [packet_shape] * len(offsets)
        scratch = [
            pltpu.VMEM((held, block_len, width), keys.dtype),
            pltpu.VMEM((held, block_len, width), values.dtype),
            pltpu.VMEM(query.shape, query.dtype),
            pltpu.VMEM(time_bucket.shape, jnp.int32),
            pltpu.VMEM(action.shape, jnp.int32),
            pltpu.VMEM(time_bias.shape[::-1], f32),
            pltpu.VMEM(action_bias.shape[::-1], f32),
            pltpu.VMEM((head_count, users, block_len), f32),
            pltpu.SMEM(lengths.shape, jnp.int32),
            pltpu.SemaphoreType.DMA((2, steps)),
            pltpu.SemaphoreType.DMA((6,)),
        ]
        if with_own:
            operands += [new_key, new_value, gate, norm_gain]
            outputs += [packet_shape, jax.ShapeDtypeStruct((row_count, width), f32)]
            scratch += [
                pltpu.VMEM((local_users, cands, width), new_key.dtype),
                pltpu.VMEM((local_users, cands, width), new_value.dtype),
                pltpu.VMEM((local_users, cands, width), gate.dtype),
                pltpu.VMEM(norm_gain.shape, f32),
                pltpu.SemaphoreType.DMA((4,)),
            ]
        return pl.pallas_call(
            functools.partial(
                attend_kernel,
                offsets=offsets,
                seq_count=seq_count,
                with_own=with_own,
                step_users=step_users,
                ahead=AHEAD,
            ),
            out_shape=tuple(outputs),
            in_specs=[hbm_spec] * len(operands),
            out_specs=tuple([vmem_spec] * len(outputs)),
            scratch_shapes=scratch,
            compiler_params=pltpu.CompilerParams(vmem_limit_bytes=held_bytes + (8 << 20)),
            name="attend",
        )(*[pltpu.with_memory_space_constraint(operand, pltpu.HBM) for operand in operands])

    order = list(reversed(range(seq_count)))
    cut = len(order) // 2 if SPLIT else 0
    received = []
    for offsets, with_own in ((order[:cut], False), (order[cut:], True)):
        if not offsets:
            continue
        results = attend(tuple(offsets), with_own)
        for offset, packet in zip(offsets, results):
            received.append(exchange(packet, "seq", offset) if offset else packet)
        if with_own:
            received.append(results[len(offsets)])
            gated = results[len(offsets) + 1]
    sends = pl.pallas_call(
        functools.partial(
            project_kernel, cands=cands, source_count=len(received), head_axis=head_axis
        ),
        out_shape=tuple(
            [jax.ShapeDtypeStruct((row_count + SUBLANES, out_cols), f32)] * head_axis
        ),
        in_specs=[vmem_spec] * (len(received) + 2),
        out_specs=tuple([vmem_spec] * head_axis),
        compiler_params=pltpu.CompilerParams(vmem_limit_bytes=8 << 20),
        name="project",
    )(*received, gated, w_out)
    parts = [
        exchange(sends[offset], "head", offset) if offset else sends[offset]
        for offset in reversed(range(head_axis))
    ]
    return pl.pallas_call(
        functools.partial(finish_kernel, full_width=width * head_axis),
        out_shape=jax.ShapeDtypeStruct((local_users, cands, out_cols), jnp.bfloat16),
        in_specs=[vmem_spec] * head_axis,
        out_specs=vmem_spec,
        compiler_params=pltpu.CompilerParams(vmem_limit_bytes=4 << 20),
        name="finish",
    )(*parts)


def solution(mesh):
    placed = (
        P("groups", None, "head"),
        P("groups", None, "head"),
        P("groups", None, "head"),
        P("groups", "seq", "head"),
        P("groups", "seq", "head"),
        P("groups"),
        P("groups", "seq"),
        P("groups", "seq"),
        P(None, "head"),
        P(None, "head"),
        P("groups", None, "head"),
        P("head"),
        P("head", None),
    )
    return jax.shard_map(
        body,
        mesh=mesh,
        in_specs=placed,
        out_specs=P(("groups", "seq"), None, "head"),
        check_vma=False,
    )
```

```python
import functools
import math

import jax
import jax.numpy as jnp
from jax import lax
from jax.experimental import pallas as pl
from jax.experimental.pallas import tpu as pltpu
from jax.sharding import PartitionSpec as P

LANES = 128
SUBLANES = 8
MASKED = -1e30
HALF = LANES // 2
STEP_USERS = 4
AHEAD = 2
SPLIT = True


def partner_of(rank, offset, size):
    if size & (size - 1) == 0:
        return rank ^ offset
    return (rank + offset) % size


def exchange(packet, axis, offset):
    size = lax.axis_size(axis)
    pairs = [(rank, partner_of(rank, offset, size)) for rank in range(size)]
    return lax.ppermute(packet, axis, pairs)


def column_to_row(column, first_lane):
    rows = column.shape[0]
    row_id = lax.broadcasted_iota(jnp.int32, (rows, LANES), 0)
    lane_id = lax.broadcasted_iota(jnp.int32, (rows, LANES), 1)
    return jnp.sum(
        jnp.where(lane_id == row_id + first_lane, column, 0.0), axis=0, keepdims=True
    )


def attend_kernel(*refs, offsets, seq_count, with_own, step_users, ahead):
    refs = list(refs)
    take = lambda count: [refs.pop(0) for _ in range(count)]
    (
        query_hbm,
        keys_hbm,
        values_hbm,
        lengths_hbm,
        time_bucket_hbm,
        action_hbm,
        time_bias_hbm,
        action_bias_hbm,
    ) = take(8)
    if with_own:
        new_key_hbm, new_value_hbm, gate_hbm, gain_hbm = take(4)
    packets = take(len(offsets))
    if with_own:
        self_ref, gated_ref = take(2)
    (
        key_buf,
        value_buf,
        query_buf,
        bucket_buf,
        action_buf,
        time_table,
        action_table,
        bias_buf,
        lengths_smem,
        block_sems,
        small_sems,
    ) = take(11)
    if with_own:
        new_key_buf, new_value_buf, gate_buf, gain_buf, own_sems = take(5)
    _, block_len, width = key_buf.shape
    users, cands, _ = query_buf.shape
    head_count = time_table.shape[0]
    head_size = width // head_count
    group_rows = head_count * cands
    local_users = users // seq_count
    stat_row = local_users * group_rows
    scale = 1.0 / math.sqrt(head_size)
    rank = lax.axis_index("seq")
    first_user = rank * local_users

    small = [
        pltpu.make_async_copy(source, target, small_sems.at[number])
        for number, (source, target) in enumerate(
            [
                (lengths_hbm, lengths_smem),
                (time_bias_hbm, time_table),
                (action_bias_hbm, action_table),
                (time_bucket_hbm, bucket_buf),
                (action_hbm, action_buf),
                (query_hbm, query_buf),
            ]
        )
    ]
    late = []
    if with_own:
        own_rows = pl.ds(first_user, local_users)
        late = [
            pltpu.make_async_copy(source, target, own_sems.at[number])
            for number, (source, target) in enumerate(
                [
                    (new_key_hbm.at[own_rows], new_key_buf),
                    (new_value_hbm.at[own_rows], new_value_buf),
                    (gate_hbm.at[own_rows], gate_buf),
                    (gain_hbm, gain_buf),
                ]
            )
        ]

    steps = [
        (slot, place)
        for slot in range(len(offsets))
        for place in range(0, local_users, step_users)
    ]

    def copies(number):
        slot, place = steps[number]
        source = pl.ds(
            partner_of(rank, offsets[slot], seq_count) * local_users + place, step_users
        )
        target = pl.ds(number * step_users, step_users)
        return (
            pltpu.make_async_copy(
                keys_hbm.at[source], key_buf.at[target], block_sems.at[0, number]
            ),
            pltpu.make_async_copy(
                values_hbm.at[source], value_buf.at[target], block_sems.at[1, number]
            ),
        )

    for copy in small:
        copy.start()
    for number in range(min(ahead, len(steps))):
        for copy in copies(number):
            copy.start()
    for copy in late:
        copy.start()
    for copy in small:
        copy.wait()

    lane_id = lax.broadcasted_iota(jnp.int32, (SUBLANES, LANES), 1)
    sub_id = lax.broadcasted_iota(jnp.int32, (SUBLANES, LANES), 0)

    def padded_table(ref, head):
        row = ref[head : head + 1, :]
        missing = LANES - row.shape[1]
        row = jnp.concatenate([row, jnp.zeros((1, missing), row.dtype)], axis=1)
        return jnp.broadcast_to(row, (SUBLANES, LANES))

    time_rows = [padded_table(time_table, head) for head in range(head_count)]
    action_rows = [padded_table(action_table, head) for head in range(head_count)]
    for group in range(users // SUBLANES):
        limit = jnp.zeros((SUBLANES, LANES), jnp.int32)
        for member in range(SUBLANES):
            left = lengths_smem[group * SUBLANES + member] - rank * block_len
            limit = jnp.where(sub_id == member, left, limit)
        rows = slice(group * SUBLANES, (group + 1) * SUBLANES)
        for piece in range(block_len // LANES):
            cols = slice(piece * LANES, (piece + 1) * LANES)
            bucket = bucket_buf[rows, cols]
            kind = action_buf[rows, cols]
            valid = lane_id + piece * LANES < limit
            for head in range(head_count):
                bias = jnp.take_along_axis(
                    time_rows[head], bucket, axis=1, mode="promise_in_bounds"
                ) + jnp.take_along_axis(
                    action_rows[head], kind, axis=1, mode="promise_in_bounds"
                )
                bias_buf[head, rows, cols] = jnp.where(valid, bias, MASKED)

    col_head = lax.broadcasted_iota(jnp.int32, (cands, width), 1) // head_size

    def score_user(slot, place, held):
        user = partner_of(rank, offsets[slot], seq_count) * local_users + place
        query = query_buf[user]
        stacked = jnp.concatenate(
            [
                jnp.where(col_head == head, query, jnp.zeros_like(query))
                for head in range(head_count)
            ],
            axis=0,
        )
        scores = jnp.concatenate(
            [
                lax.dot_general(
                    query[:, head * head_size : (head + 1) * head_size],
                    key_buf[held, :, head * head_size : (head + 1) * head_size],
                    (((1,), (1,)), ((), ())),
                    preferred_element_type=jnp.float32,
                )
                for head in range(head_count)
            ],
            axis=0,
        )
        biases = jnp.concatenate(
            [
                jnp.broadcast_to(bias_buf[head, pl.ds(user, 1), :], (cands, block_len))
                for head in range(head_count)
            ],
            axis=0,
        )
        return scores * scale + biases

    def weigh_user(slot, place, held, scores):
        block_max = jnp.max(scores, axis=1, keepdims=True)
        weights = jnp.exp(scores - block_max)
        block_sum = jnp.sum(weights, axis=1, keepdims=True)
        block_acc = jnp.dot(
            weights.astype(jnp.bfloat16), value_buf[held], preferred_element_type=jnp.float32
        )
        packet = packets[slot]
        for head in range(head_count):
            first = place * group_rows + head * cands
            packet[first : first + cands, :] = block_acc[
                head * cands : (head + 1) * cands, head * head_size : (head + 1) * head_size
            ]
        packet[stat_row + place : stat_row + place + 1, :] = column_to_row(
            block_max, 0
        ) + column_to_row(block_sum, HALF)

    pending = []
    for number, (slot, place) in enumerate(steps):
        copies(number)[0].wait()
        if number:
            copies(number - 1)[1].wait()
        if number + ahead < len(steps):
            for copy in copies(number + ahead):
                copy.start()
        scored = []
        for member in range(step_users):
            task = (slot, place + member, number * step_users + member)
            scored.append(task + (score_user(*task),))
        for task in pending:
            weigh_user(*task)
        pending = scored
    copies(len(steps) - 1)[1].wait()
    for task in pending:
        weigh_user(*task)

    if not with_own:
        return
    for copy in late:
        copy.wait()
    gain = gain_buf[...].reshape(1, width)
    for place in range(local_users):
        own_query = query_buf[first_user + place].astype(jnp.float32)
        own_key = new_key_buf[place].astype(jnp.float32)
        own_value = new_value_buf[place].astype(jnp.float32)
        gate = gate_buf[place].astype(jnp.float32)
        product = own_query * own_key
        row = jnp.zeros((1, LANES), jnp.float32)
        for head in range(head_count):
            cols = slice(head * head_size, (head + 1) * head_size)
            own = jnp.sum(product[:, cols], axis=1, keepdims=True) * scale
            row = row + column_to_row(own, head * cands)
            row = row + column_to_row(jnp.ones_like(own), HALF + head * cands)
            first = place * group_rows + head * cands
            self_ref[first : first + cands, :] = own_value[:, cols]
        self_ref[stat_row + place : stat_row + place + 1, :] = row
        gated_ref[place * cands : (place + 1) * cands, :] = gain * (gate / (1.0 + jnp.exp(-gate)))


def project_kernel(*refs, cands, source_count, head_axis):
    packets = refs[:source_count]
    gated_ref, w_ref = refs[source_count : source_count + 2]
    sends = refs[source_count + 2 :]
    head_size = packets[0].shape[1]
    row_count, width = gated_ref.shape
    head_count = width // head_size
    local_users = row_count // cands
    group_rows = head_count * cands
    stat_row = local_users * group_rows
    out_cols = w_ref.shape[1] // head_axis
    rank = lax.axis_index("head")

    stats = [
        packet[stat_row + place : stat_row + place + 1, :]
        for place in range(local_users)
        for packet in packets
    ]
    stats.append(jnp.zeros((LANES - len(stats), LANES), jnp.float32))
    columns = jnp.concatenate(stats, axis=0).T

    hidden = []
    square_row = jnp.zeros((1, LANES), jnp.float32)
    for place in range(local_users):
        span = slice(place * source_count, (place + 1) * source_count)
        maxima = columns[0:group_rows, span]
        sums = columns[HALF : HALF + group_rows, span]
        top = jnp.max(maxima, axis=1, keepdims=True)
        factors = jnp.exp(maxima - top)
        factors = factors / jnp.sum(factors * sums, axis=1, keepdims=True)
        rows = slice(place * group_rows, (place + 1) * group_rows)
        attended = factors[:, 0:1] * packets[0][rows, :]
        for source in range(1, source_count):
            attended = attended + factors[:, source : source + 1] * packets[source][rows, :]
        wide = jnp.concatenate(
            [attended[head * cands : (head + 1) * cands, :] for head in range(head_count)], axis=1
        )
        square = jnp.sum(wide * wide, axis=1, keepdims=True)
        square_row = square_row + column_to_row(square, place * cands)
        gated = gated_ref[place * cands : (place + 1) * cands, :]
        hidden.append((wide * gated).astype(jnp.bfloat16))
    hidden = jnp.concatenate(hidden, axis=0)
    for offset in reversed(range(head_axis)):
        first = pl.multiple_of(partner_of(rank, offset, head_axis) * out_cols, LANES)
        sends[offset][0:row_count, :] = jnp.dot(
            hidden, w_ref[:, pl.ds(first, out_cols)], preferred_element_type=jnp.float32
        )
        sends[offset][row_count : row_count + 1, 0:LANES] = square_row


def finish_kernel(*refs, full_width):
    parts, out_ref = refs[:-1], refs[-1]
    local_users, cands, _ = out_ref.shape
    row_count = local_users * cands
    total = parts[0][0:row_count, :]
    square_row = parts[0][row_count : row_count + 1, 0:LANES]
    for part in parts[1:]:
        total = total + part[0:row_count, :]
        square_row = square_row + part[row_count : row_count + 1, 0:LANES]
    row_id = lax.broadcasted_iota(jnp.int32, (row_count, LANES), 0)
    lane_id = lax.broadcasted_iota(jnp.int32, (row_count, LANES), 1)
    squares = jnp.sum(jnp.where(lane_id == row_id, square_row, 0.0), axis=1, keepdims=True)
    factor = 1.0 / jnp.sqrt(squares / full_width + 1e-06)
    result = (total * factor).astype(out_ref.dtype)
    for place in range(local_users):
        out_ref[place] = result[place * cands : (place + 1) * cands, :]


def body(
    query,
    new_key,
    new_value,
    keys,
    values,
    lengths,
    time_bucket,
    action,
    time_bias,
    action_bias,
    gate,
    norm_gain,
    w_out,
):
    users, block_len, width = keys.shape
    cands = query.shape[1]
    head_count = time_bias.shape[1]
    head_size = width // head_count
    seq_count = lax.axis_size("seq")
    head_axis = lax.axis_size("head")
    local_users = users // seq_count
    row_count = local_users * cands
    packet_rows = local_users * head_count * cands + SUBLANES
    out_cols = w_out.shape[1] // head_axis
    f32 = jnp.float32
    hbm_spec = pl.BlockSpec(memory_space=pltpu.HBM)
    vmem_spec = pl.BlockSpec(memory_space=pltpu.VMEM)
    packet_shape = jax.ShapeDtypeStruct((packet_rows, head_size), f32)
    step_users = math.gcd(local_users, STEP_USERS)

    def attend(offsets, with_own):
        held = len(offsets) * local_users
        steps = held // step_users
        held_bytes = 2 * held * block_len * width * keys.dtype.itemsize
        operands = [
            query, keys, values, lengths, time_bucket, action, time_bias.T, action_bias.T
        ]
        outputs = [packet_shape] * len(offsets)
        scratch = [
            pltpu.VMEM((held, block_len, width), keys.dtype),
            pltpu.VMEM((held, block_len, width), values.dtype),
            pltpu.VMEM(query.shape, query.dtype),
            pltpu.VMEM(time_bucket.shape, jnp.int32),
            pltpu.VMEM(action.shape, jnp.int32),
            pltpu.VMEM(time_bias.shape[::-1], f32),
            pltpu.VMEM(action_bias.shape[::-1], f32),
            pltpu.VMEM((head_count, users, block_len), f32),
            pltpu.SMEM(lengths.shape, jnp.int32),
            pltpu.SemaphoreType.DMA((2, steps)),
            pltpu.SemaphoreType.DMA((6,)),
        ]
        if with_own:
            operands += [new_key, new_value, gate, norm_gain]
            outputs += [packet_shape, jax.ShapeDtypeStruct((row_count, width), f32)]
            scratch += [
                pltpu.VMEM((local_users, cands, width), new_key.dtype),
                pltpu.VMEM((local_users, cands, width), new_value.dtype),
                pltpu.VMEM((local_users, cands, width), gate.dtype),
                pltpu.VMEM(norm_gain.shape, f32),
                pltpu.SemaphoreType.DMA((4,)),
            ]
        return pl.pallas_call(
            functools.partial(
                attend_kernel,
                offsets=offsets,
                seq_count=seq_count,
                with_own=with_own,
                step_users=step_users,
                ahead=AHEAD,
            ),
            out_shape=tuple(outputs),
            in_specs=[hbm_spec] * len(operands),
            out_specs=tuple([vmem_spec] * len(outputs)),
            scratch_shapes=scratch,
            compiler_params=pltpu.CompilerParams(vmem_limit_bytes=held_bytes + (8 << 20)),
            name="attend",
        )(*[pltpu.with_memory_space_constraint(operand, pltpu.HBM) for operand in operands])

    order = list(reversed(range(seq_count)))
    cut = len(order) - 1 if SPLIT else 0
    received = []
    for offsets, with_own in ((order[:cut], False), (order[cut:], True)):
        if not offsets:
            continue
        results = attend(tuple(offsets), with_own)
        for offset, packet in zip(offsets, results):
            received.append(exchange(packet, "seq", offset) if offset else packet)
        if with_own:
            received.append(results[len(offsets)])
            gated = results[len(offsets) + 1]
    sends = pl.pallas_call(
        functools.partial(
            project_kernel, cands=cands, source_count=len(received), head_axis=head_axis
        ),
        out_shape=tuple(
            [jax.ShapeDtypeStruct((row_count + SUBLANES, out_cols), f32)] * head_axis
        ),
        in_specs=[vmem_spec] * (len(received) + 2),
        out_specs=tuple([vmem_spec] * head_axis),
        compiler_params=pltpu.CompilerParams(vmem_limit_bytes=8 << 20),
        name="project",
    )(*received, gated, w_out)
    parts = [
        exchange(sends[offset], "head", offset) if offset else sends[offset]
        for offset in reversed(range(head_axis))
    ]
    return pl.pallas_call(
        functools.partial(finish_kernel, full_width=width * head_axis),
        out_shape=jax.ShapeDtypeStruct((local_users, cands, out_cols), jnp.bfloat16),
        in_specs=[vmem_spec] * head_axis,
        out_specs=vmem_spec,
        compiler_params=pltpu.CompilerParams(vmem_limit_bytes=4 << 20),
        name="finish",
    )(*parts)


def solution(mesh):
    placed = (
        P("groups", None, "head"),
        P("groups", None, "head"),
        P("groups", None, "head"),
        P("groups", "seq", "head"),
        P("groups", "seq", "head"),
        P("groups"),
        P("groups", "seq"),
        P("groups", "seq"),
        P(None, "head"),
        P(None, "head"),
        P("groups", None, "head"),
        P("head"),
        P("head", None),
    )
    return jax.shard_map(
        body,
        mesh=mesh,
        in_specs=placed,
        out_specs=P(("groups", "seq"), None, "head"),
        check_vma=False,
    )
```
